32 devices in a mesh: dp: 4 (over y, z), tp: 8 (over x, core).
Axes of the slice: x: 4, y: 2, z: 2, core: 2. Of those that a mesh axis runs over, the one named last changes fastest.
The devices are a block of a 4x4x8 slice.
Arguments:
- hidden_in: bfloat16 [4, 4096, 1024], P('dp', 'tp'), parts along dimension 0
- norms: float32 [2, 4, 1024], replicated
- w_qkv: bfloat16 [2, 1024, 3, 16, 64], P(None, None, None, 'tp')
- w_out: bfloat16 [2, 16, 64, 1024], P(None, 'tp')
- b_out: float32 [2, 1024], replicated
- w_up: bfloat16 [2, 1024, 4096], P(None, None, 'tp')
- b_up: float32 [2, 4096], P(None, 'tp')
- w_down: bfloat16 [2, 4096, 1024], P(None, 'tp')
- b_down: float32 [2, 1024], replicated
Outputs:
- output: bfloat16 [4, 4096, 1024], P('dp', 'tp'), parts along dimension 0
There are 4 independent parts. The reference program is written for one: setup_inputs(seed, part) draws one part's arguments, and reference() takes and returns one part's arrays. A program takes and returns all parts, laid end to end along the dimension named above; an argument that names none is the same for every part.
All inputs are finite; a program needn't handle non-finite values.
Results may differ from the reference program's by a relative error of at most 0.0109788.
Values are sent between devices in bfloat16 or wider.
A program may use at most 768 MiB of HBM per device.

```python
import math
import jax
import jax.numpy as jnp
from jax import lax

N_BATCH = 1
SEQ_LEN = 4096
N_HEADS = 16
HEAD_DIM = 64
FF_DIM = 4096
N_LAYERS = 2

MODEL_DIM = N_HEADS * HEAD_DIM
LN_EPS = 1e-5


def setup_inputs(seed: int = 0, part: int = 0) -> dict:
    base_key = jax.random.key(seed)
    keys = jax.random.split(base_key, 9)
    part_key = jax.random.fold_in(keys[0], part)
    tok_key, scale_key = jax.random.split(part_key)
    tok_scale = jnp.exp(0.4 * jax.random.normal(scale_key, (N_BATCH, SEQ_LEN, 1), jnp.float32))
    hidden_in = (jax.random.normal(tok_key, (N_BATCH, SEQ_LEN, MODEL_DIM), jnp.float32) * tok_scale).astype(jnp.bfloat16)
    norm_base = jnp.array([1.0, 0.0, 1.0, 0.0], jnp.float32)[None, :, None]
    norms = norm_base + 0.2 * jax.random.normal(keys[1], (N_LAYERS, 4, MODEL_DIM), jnp.float32)
    qk_gain = (math.log(SEQ_LEN) / 2.0) ** 0.25
    slot_gain = jnp.array([qk_gain, qk_gain, 1.0], jnp.float32)[None, None, :, None, None]
    w_qkv = (jax.random.normal(keys[2], (N_LAYERS, MODEL_DIM, 3, N_HEADS, HEAD_DIM), jnp.float32) * slot_gain * MODEL_DIM ** -0.5).astype(jnp.bfloat16)
    out_gain = 0.7 * SEQ_LEN ** 0.25 * MODEL_DIM ** -0.5
    w_out = (jax.random.normal(keys[3], (N_LAYERS, N_HEADS, HEAD_DIM, MODEL_DIM), jnp.float32) * out_gain).astype(jnp.bfloat16)
    b_out = 0.2 * jax.random.normal(keys[4], (N_LAYERS, MODEL_DIM), jnp.float32)
    w_up = (jax.random.normal(keys[5], (N_LAYERS, MODEL_DIM, FF_DIM), jnp.float32) * MODEL_DIM ** -0.5).astype(jnp.bfloat16)
    b_up = 0.3 * jax.random.normal(keys[6], (N_LAYERS, FF_DIM), jnp.float32)
    w_down = (jax.random.normal(keys[7], (N_LAYERS, FF_DIM, MODEL_DIM), jnp.float32) * FF_DIM ** -0.5).astype(jnp.bfloat16)
    b_down = 0.2 * jax.random.normal(keys[8], (N_LAYERS, MODEL_DIM), jnp.float32)
    return {'hidden_in': hidden_in, 'norms': norms, 'w_qkv': w_qkv, 'w_out': w_out, 'b_out': b_out, 'w_up': w_up, 'b_up': b_up, 'w_down': w_down, 'b_down': b_down}


def layer_norm(rows, gain, shift):
    row_mean = jnp.mean(rows, axis=-1, keepdims=True)
    centred = rows - row_mean
    row_var = jnp.mean(centred * centred, axis=-1, keepdims=True)
    return (centred * lax.rsqrt(row_var + LN_EPS) * gain + shift).astype(jnp.bfloat16)


def one_head(head_qkv):
    queries = head_qkv[:, 0].astype(jnp.float32)
    keys_h = head_qkv[:, 1].astype(jnp.float32)
    values_h = head_qkv[:, 2].astype(jnp.float32)
    scores = jnp.einsum('bqe,bke->bqk', queries, keys_h) * HEAD_DIM ** -0.5
    attn_prob = jax.nn.softmax(scores, axis=-1).astype(jnp.bfloat16)
    return jnp.einsum('bqk,bke->bqe', attn_prob.astype(jnp.float32), values_h).astype(jnp.bfloat16)


def one_layer(residual, params):
    norm_l, wqkv_l, wout_l, bout_l, wup_l, bup_l, wdown_l, bdown_l = params
    normed = layer_norm(residual, norm_l[0], norm_l[1])
    qkv_heads = jnp.einsum('bsd,dthe->hbtse', normed.astype(jnp.float32), wqkv_l.astype(jnp.float32)).astype(jnp.bfloat16)
    attn_rows = lax.map(one_head, qkv_heads)
    attn_out = jnp.einsum('hbse,hed->bsd', attn_rows.astype(jnp.float32), wout_l.astype(jnp.float32))
    residual = residual + attn_out + bout_l
    normed2 = layer_norm(residual, norm_l[2], norm_l[3])
    hidden = jnp.einsum('bsd,df->bsf', normed2.astype(jnp.float32), wup_l.astype(jnp.float32)) + bup_l
    gelu_out = jax.nn.gelu(hidden, approximate=True).astype(jnp.bfloat16)
    mlp_out = jnp.einsum('bsf,fd->bsd', gelu_out.astype(jnp.float32), wdown_l.astype(jnp.float32))
    residual = residual + mlp_out + bdown_l
    return residual, None


def reference(hidden_in, norms, w_qkv, w_out, b_out, w_up, b_up, w_down, b_down):
    residual, unused = lax.scan(one_layer, hidden_in.astype(jnp.float32), (norms, w_qkv, w_out, b_out, w_up, b_up, w_down, b_down))
    return residual.astype(jnp.bfloat16)
```

```python
import functools
import jax
import jax.numpy as jnp
from jax import lax
from jax.experimental import pallas as pl
from jax.experimental.pallas import tpu as pltpu
from jax.sharding import PartitionSpec as P

LN_EPS = 1e-5
LOG2E = 1.4426950408889634
NT = (((1,), (1,)), ((), ()))
VMEM_LIMIT = 60 * 2**20


def layer_norm(rows, gain, shift):
    row_mean = jnp.mean(rows, axis=-1, keepdims=True)
    centred = rows - row_mean
    row_var = jnp.mean(centred * centred, axis=-1, keepdims=True)
    return (centred * lax.rsqrt(row_var + LN_EPS) * gain + shift).astype(jnp.bfloat16)


def whole():
    return pl.BlockSpec(memory_space=pltpu.VMEM)


def norm_kernel(rows_ref, norms_ref, out_ref):
    out_ref[...] = layer_norm(rows_ref[...].astype(jnp.float32), norms_ref[0:1, :], norms_ref[1:2, :])


def norm_rows(rows, norms):
    return pl.pallas_call(
        norm_kernel,
        out_shape=jax.ShapeDtypeStruct(rows.shape, jnp.bfloat16),
        in_specs=[whole()] * 2,
        out_specs=whole(),
        cost_estimate=pl.CostEstimate(flops=10 * rows.size, bytes_accessed=4 * rows.size, transcendentals=0),
        name='norm_rows',
    )(rows, norms)


def attn_kernel(head_dim, qt, kc, x_ref, wqk_ref, wvt_ref, o_ref, q_s, k_s, vt_s, s_s, acc_s):
    seq = x_ref.shape[0]
    pair = 2 * head_dim
    rows = 512
    n_heads = 2
    scale = head_dim ** -0.5 * LOG2E
    vt_s[:, head_dim:, :] = jnp.ones((n_heads, vt_s.shape[1] - head_dim, seq), jnp.bfloat16)

    @pl.loop(0, seq // rows)
    def _(i):
        at = pl.ds(pl.multiple_of(i * rows, rows), rows)
        xr = x_ref[at, :]
        qk = jnp.dot(xr, wqk_ref[...], preferred_element_type=jnp.float32)
        q_s[at, :] = qk[:, :pair].astype(jnp.bfloat16)
        k_s[at, :] = qk[:, pair:].astype(jnp.bfloat16)
        vt = lax.dot_general(wvt_ref[...], xr, NT, preferred_element_type=jnp.float32).astype(jnp.bfloat16)
        for h in range(n_heads):
            vt_s[h, :head_dim, at] = vt[h * head_dim:(h + 1) * head_dim]

    n_tiles = seq // qt
    n_chunks = seq // kc

    def masked_q(j):
        q = q_s[pl.ds(pl.multiple_of(j * qt, qt), qt), :]
        lane = lax.broadcasted_iota(jnp.int32, q.shape, 1)
        zero = jnp.zeros_like(q)
        return jnp.concatenate([jnp.where(lane < head_dim, q, zero), jnp.where(lane >= head_dim, q, zero)], axis=0)

    def scores(c, qm):
        return lax.dot_general(k_s[c * kc:(c + 1) * kc, :], qm, NT, preferred_element_type=jnp.float32)

    def fold(s):
        return jnp.max(s.reshape(kc // 8, 8, s.shape[1]), axis=0)

    qm0 = masked_q(0)
    mx = jnp.full((8, 2 * qt), -jnp.inf, jnp.float32)
    for c in range(n_chunks):
        s = scores(c, qm0)
        s_s[0, c * kc:(c + 1) * kc, :] = s
        mx = jnp.maximum(mx, fold(s))
    m0 = jnp.max(mx, axis=0, keepdims=True) * scale

    def tile(j, m):
        slot = 0
        qm = masked_q(j)
        mx = jnp.full((8, 2 * qt), -jnp.inf, jnp.float32)
        for c in range(n_chunks):
            at = slice(c * kc, (c + 1) * kc)
            s = scores(c, qm)
            s_s[0, at, :] = s
            mx = jnp.maximum(mx, fold(s))
        m = jnp.max(mx, axis=0, keepdims=True) * scale
        for c in range(n_chunks):
            at = slice(c * kc, (c + 1) * kc)
            p = jnp.exp2(s_s[slot, at, :] * scale - m).astype(jnp.bfloat16)
            for h in range(n_heads):
                part = jnp.dot(vt_s[h, :, at], p[:, h * qt:(h + 1) * qt], preferred_element_type=jnp.float32)
                if c == 0:
                    acc_s[h] = part
                else:
                    acc_s[h] += part
        ots = []
        for h in range(n_heads):
            acc = acc_s[h]
            ots.append(acc[:head_dim] / acc[head_dim:head_dim + 1])
        ot = jnp.concatenate(ots, axis=0)
        o_ref[pl.ds(pl.multiple_of(j * qt, qt), qt), :] = ot.T.astype(jnp.bfloat16)
        return jnp.max(mx, axis=0, keepdims=True) * scale

    lax.fori_loop(0, n_tiles, tile, m0)

def attn(x, wqk, wvt, head_dim, qt=256, kc=512):
    seq = x.shape[0]
    return pl.pallas_call(
        functools.partial(attn_kernel, head_dim, qt, kc),
        out_shape=jax.ShapeDtypeStruct((seq, 2 * head_dim), jnp.bfloat16),
        in_specs=[pl.BlockSpec(memory_space=pltpu.VMEM)] * 3,
        out_specs=pl.BlockSpec(memory_space=pltpu.VMEM),
        scratch_shapes=[
            pltpu.VMEM((seq, 2 * head_dim), jnp.bfloat16),
            pltpu.VMEM((seq, 2 * head_dim), jnp.bfloat16),
            pltpu.VMEM((2, head_dim + 16, seq), jnp.bfloat16),
            pltpu.VMEM((2, seq, 2 * qt), jnp.float32),
            pltpu.VMEM((2, head_dim + 16, qt), jnp.float32),
        ],
        compiler_params=pltpu.CompilerParams(vmem_limit_bytes=60 * 2**20),
        cost_estimate=pl.CostEstimate(flops=12 * 10**9, bytes_accessed=10 * 2**20, transcendentals=2 * seq * seq),
        name="attn",
    )(x, wqk, wvt)


def mlp_kernel(layer, last, o_ref, res_ref, norms_ref, b_out_ref, b_down_ref, w_out_ref, w_up_ref, b_up_ref, w_down_ref, r_ref, h_ref, h2_s):
    step = pl.program_id(0)
    base = 4 * layer

    @pl.when(step == 0)
    def _():
        heads = jnp.concatenate([o_ref[i] for i in range(o_ref.shape[0])], axis=1)
        attn_out = jnp.dot(heads, w_out_ref[...], preferred_element_type=jnp.float32)
        r = res_ref[...].astype(jnp.float32) + attn_out + b_out_ref[layer:layer + 1, :]
        r_ref[...] = r
        h2_s[...] = layer_norm(r, norms_ref[base + 2:base + 3, :], norms_ref[base + 3:base + 4, :])

    hidden = jnp.dot(h2_s[...], w_up_ref[...], preferred_element_type=jnp.float32) + b_up_ref[...]
    gelu_out = jax.nn.gelu(hidden, approximate=True).astype(jnp.bfloat16)
    r_ref[...] += jnp.dot(gelu_out, w_down_ref[...], preferred_element_type=jnp.float32)

    @pl.when(step == pl.num_programs(0) - 1)
    def _():
        r = r_ref[...] + b_down_ref[layer:layer + 1, :]
        if last:
            h_ref[...] = r.astype(jnp.bfloat16)
        else:
            r_ref[...] = r
            h_ref[...] = layer_norm(r, norms_ref[base + 4:base + 5, :], norms_ref[base + 5:base + 6, :])


def mlp(layer, last, o, res, norms, b_out, b_down, w_out, w_up, b_up, w_down):
    n, width, ff = w_up.shape
    rows = res.shape[0]

    def whole_block(a):
        return pl.BlockSpec(a.shape, lambda i: (0,) * a.ndim)

    return pl.pallas_call(
        functools.partial(mlp_kernel, layer, last),
        grid=(n,),
        out_shape=(jax.ShapeDtypeStruct((rows, width), jnp.float32), jax.ShapeDtypeStruct((rows, width), jnp.bfloat16)),
        in_specs=[whole_block(o), whole_block(res), whole_block(norms), whole_block(b_out), whole_block(b_down), whole_block(w_out),
                  pl.BlockSpec((None, width, ff), lambda i: (i, 0, 0)),
                  pl.BlockSpec((None, None, 1, ff), lambda i: (i, layer, 0, 0)),
                  pl.BlockSpec((None, ff, width), lambda i: (i, 0, 0))],
        out_specs=(pl.BlockSpec((rows, width), lambda i: (0, 0)), pl.BlockSpec((rows, width), lambda i: (0, 0))),
        scratch_shapes=[pltpu.VMEM((rows, width), jnp.bfloat16)],
        compiler_params=pltpu.CompilerParams(dimension_semantics=('arbitrary',), vmem_limit_bytes=VMEM_LIMIT),
        cost_estimate=pl.CostEstimate(flops=4 * rows * width * ff * n, bytes_accessed=4 * n * width * ff, transcendentals=rows * n * ff),
        name='mlp',
    )(o, res, norms, b_out, b_down, w_out, w_up, b_up, w_down)


def solution(mesh):
    group_size = mesh.shape['tp']

    def local_layers(hidden_in, norms, w_qkv, w_out, b_out, w_up, b_up, w_down, b_down):
        n_layers, width, slots, heads_loc, head_dim = w_qkv.shape
        rows = hidden_in.shape[1]
        pair = heads_loc * head_dim
        norms = norms.reshape(n_layers * 4, width)
        residual = hidden_in[0]
        normed = norm_rows(residual, norms)
        b_up_all = lax.all_gather(b_up.reshape(n_layers, 1, -1), 'tp')
        for layer in range(n_layers):
            w_l = w_qkv[layer].reshape(width, slots * pair)
            wqk, wvt = w_l[:, :2 * pair], w_l[:, 2 * pair:].T
            x = lax.all_gather(normed, 'tp', axis=0, tiled=True)
            x, w_out_l, w_up_l, w_down_l = lax.optimization_barrier((x, w_out[layer].reshape(pair, width), w_up[layer], w_down[layer]))
            w_out_all = lax.all_gather(w_out_l, 'tp', axis=0, tiled=True)
            w_up_all = lax.all_gather(w_up_l, 'tp')
            w_down_all = lax.all_gather(w_down_l, 'tp')
            o = attn(x, wqk, wvt, head_dim)
            o = lax.all_to_all(o.reshape(group_size, rows, pair), 'tp', 0, 0)
            residual, normed = mlp(layer, layer == n_layers - 1, o, residual, norms, b_out, b_down, w_out_all, w_up_all, b_up_all, w_down_all)
        return normed[None]

    in_specs = (P('dp', 'tp', None), P(), P(None, None, None, 'tp', None), P(None, 'tp', None, None), P(), P(None, None, 'tp'), P(None, 'tp'), P(None, 'tp', None), P())
    return jax.shard_map(local_layers, mesh=mesh, in_specs=in_specs, out_specs=P('dp', 'tp', None), check_vma=False)
```

```python
import functools
import jax
import jax.numpy as jnp
from jax import lax
from jax.experimental import pallas as pl
from jax.experimental.pallas import tpu as pltpu
from jax.sharding import PartitionSpec as P

MESH = pl.DeviceIdType.MESH
LN_EPS = 1e-5
LOG2E = 1.4426950408889634
NT = (((1,), (1,)), ((), ()))
VMEM_LIMIT = 63 * 2**20

ME, SIB, LEFT, RIGHT, OPP, SLEFT, SRIGHT, SOPP = range(8)
INVERSE = {SIB: SIB, LEFT: RIGHT, RIGHT: LEFT, OPP: OPP, SLEFT: SRIGHT, SRIGHT: SLEFT, SOPP: SOPP}
ACROSS = {ME: SIB, LEFT: SLEFT, RIGHT: SRIGHT, OPP: SOPP}
ORDER = [OPP, SOPP, LEFT, SLEFT, RIGHT, SRIGHT, SIB, ME]
PLACE = {rel: i for i, rel in enumerate(ORDER)}
PIECES = 4

Z_CHUNKS = ['zu0', 'zu1', 'zd0', 'zd1']
X_CHUNKS = Z_CHUNKS + ['cu', 'cd', 'co']
TO_RIGHT = ['zu0', 'zd0', 'co', 'zu1', 'zd1', 'cu', 'cd']
TO_LEFT = ['zu1', 'zd1', 'cu', 'zu0', 'zd0', 'cd', 'co']
RELAY_RIGHT = ['zu0', 'zd0', 'co']
RELAY_LEFT = ['zu1', 'zd1', 'cu', 'cd']


def layer_norm(rows, gain, shift):
    row_mean = jnp.mean(rows, axis=-1, keepdims=True)
    centred = rows - row_mean
    row_var = jnp.mean(centred * centred, axis=-1, keepdims=True)
    return (centred * lax.rsqrt(row_var + LN_EPS) * gain + shift).astype(jnp.bfloat16)


def whole():
    return pl.BlockSpec(memory_space=pltpu.VMEM)


def norm_kernel(rows_ref, norms_ref, out_ref):
    out_ref[...] = layer_norm(rows_ref[...].astype(jnp.float32), norms_ref[0:1, :], norms_ref[1:2, :])


def norm_rows(rows, norms):
    return pl.pallas_call(
        norm_kernel,
        out_shape=jax.ShapeDtypeStruct(rows.shape, jnp.bfloat16),
        in_specs=[whole()] * 2,
        out_specs=whole(),
        cost_estimate=pl.CostEstimate(flops=10 * rows.size, bytes_accessed=4 * rows.size, transcendentals=0),
        name='norm_rows',
    )(rows, norms)


def message_keys():
    keys = []
    for p in range(PIECES):
        keys += [('xr', p), ('xl', p), ('xs', ME, p)]
        keys += [('xs', rel, p) for rel in (LEFT, RIGHT, OPP)]
        keys += [('xrr', p)] if p < PIECES // 2 else [('xll', p)]
    keys += [('wr', c) for c in X_CHUNKS] + [('wl', c) for c in X_CHUNKS]
    keys += [('wrr', c) for c in RELAY_RIGHT] + [('wll', c) for c in RELAY_LEFT]
    keys += [('ws', a) for a in ('u', 'd', 'o')]
    for rel in (LEFT, RIGHT, OPP):
        keys += [('wfx', rel, c) for c in X_CHUNKS]
        keys += [('wz', rel, c) for c in Z_CHUNKS] + [('wfz', rel, c) for c in Z_CHUNKS]
    keys += [('o', rel) for rel in INVERSE] + [('b', rel) for rel in INVERSE]
    return keys


KEYS = {key: i for i, key in enumerate(message_keys())}


def layer_kernel(layer, last, group_size, qt, kc, h_ref, res_ref, norms_ref, b_out_ref, b_down_ref, b_up_ref, wqk_ref, wvt_ref,
                 w_out_ref, w_up_ref, w_down_ref, r_ref, hn_ref,
                 x_v, wo_v, wu_v, wd_v, bu_v, q_s, k_s, vt_s, s_s, acc_s, o_loc, o_rcv, h2_s, send_sems, recv_sems, own_sems):
    rows, width = h_ref.shape
    ff = w_up_ref.shape[-1]
    seq = q_s.shape[0]
    pair = q_s.shape[1]
    n_heads = 2
    head_dim = pair // n_heads
    scale = head_dim ** -0.5 * LOG2E
    base = 4 * layer

    me = lax.axis_index('tp')
    chip, core = me // 2, me % 2
    n_chips = group_size // 2
    parity = lax.axis_index('dp') % 2
    partner = lax.axis_index('dp') + 1 - 2 * parity

    def at(step, flip):
        return {'tp': 2 * ((chip + step) % n_chips) + (1 - core if flip else core)}

    far = n_chips // 2
    device = {SIB: at(0, True), LEFT: at(n_chips - 1, False), RIGHT: at(1, False), OPP: at(far, False),
              SLEFT: at(n_chips - 1, True), SRIGHT: at(1, True), SOPP: at(far, True)}
    pair_device = {'dp': partner, 'tp': me}

    piece_rows = rows // PIECES
    up_z, down_z = width * 7 // 32, ff * 7 // 32

    def x_at(rel, p):
        ref = h_ref if rel == ME else x_v.at[rel]
        return ref.at[p * piece_rows:(p + 1) * piece_rows, :]

    def w_at(rel, c, par):
        if c == 'co':
            return wo_v.at[rel]
        if c == 'cu':
            return wu_v.at[rel, 4 * up_z:, :]
        if c == 'cd':
            return wd_v.at[rel, 4 * down_z:, :]
        i = int(c[2])
        if c[1] == 'u':
            return wu_v.at[rel, pl.ds(pl.multiple_of(par * (2 * up_z) + i * up_z, 16), up_z), :]
        return wd_v.at[rel, pl.ds(pl.multiple_of(par * (2 * down_z) + i * down_z, 16), down_z), :]

    def message(key, receiving=False):
        kind = key[0]
        here, there = parity, 1 - parity
        if kind == 'xr':
            src, dst, dev = x_at(ME, key[1]), x_at(LEFT, key[1]), device[RIGHT]
        elif kind == 'xl':
            src, dst, dev = x_at(ME, key[1]), x_at(RIGHT, key[1]), device[LEFT]
        elif kind == 'xrr':
            src, dst, dev = x_at(LEFT, key[1]), x_at(OPP, key[1]), device[RIGHT]
        elif kind == 'xll':
            src, dst, dev = x_at(RIGHT, key[1]), x_at(OPP, key[1]), device[LEFT]
        elif kind == 'xs':
            src, dst, dev = x_at(key[1], key[2]), x_at(ACROSS[key[1]], key[2]), device[SIB]
        elif kind == 'wr':
            src, dst, dev = w_at(ME, key[1], here), w_at(LEFT, key[1], here), device[RIGHT]
        elif kind == 'wl':
            src, dst, dev = w_at(ME, key[1], here), w_at(RIGHT, key[1], here), device[LEFT]
        elif kind == 'wrr':
            src, dst, dev = w_at(LEFT, key[1], here), w_at(OPP, key[1], here), device[RIGHT]
        elif kind == 'wll':
            src, dst, dev = w_at(RIGHT, key[1], here), w_at(OPP, key[1], here), device[LEFT]
        elif kind == 'ws':
            ref = {'u': wu_v, 'd': wd_v, 'o': wo_v}[key[1]]
            src, dst, dev = ref.at[ME], ref.at[SIB], device[SIB]
        elif kind == 'wfx':
            src, dst, dev = w_at(key[1], key[2], here), w_at(ACROSS[key[1]], key[2], here), device[SIB]
        elif kind == 'wz':
            par = there if receiving else here
            src, dst, dev = w_at(key[1], key[2], par), w_at(key[1], key[2], par), pair_device
        elif kind == 'wfz':
            src, dst, dev = w_at(key[1], key[2], there), w_at(ACROSS[key[1]], key[2], there), device[SIB]
        elif kind == 'o':
            src = o_loc.at[PLACE[key[1]] * rows:(PLACE[key[1]] + 1) * rows, :]
            dst, dev = o_rcv.at[INVERSE[key[1]]], device[key[1]]
        else:
            src, dst, dev = b_up_ref, bu_v.at[INVERSE[key[1]]], device[key[1]]
        i = KEYS[key]
        return pltpu.make_async_remote_copy(src_ref=src, dst_ref=dst, send_sem=send_sems.at[i], recv_sem=recv_sems.at[i],
                                            device_id=dev, device_id_type=MESH)

    def start(*key):
        message(key).start()

    def recv(*key):
        message(key, True).wait_recv()

    def own_copies():
        return [pltpu.make_async_copy(w_up_ref.at[layer], wu_v.at[ME], own_sems.at[0]),
                pltpu.make_async_copy(w_down_ref.at[layer], wd_v.at[ME], own_sems.at[1]),
                pltpu.make_async_copy(w_out_ref.at[layer], wo_v.at[ME], own_sems.at[2])]

    for copy in own_copies():
        copy.start()
    barrier = pltpu.get_barrier_semaphore()
    peers = list(device.values()) + [pair_device]
    for dev in peers:
        pl.semaphore_signal(barrier, inc=1, device_id=dev, device_id_type=MESH)
    pl.semaphore_wait(barrier, len(peers))

    right_order = list(range(PIECES))
    left_order = right_order[PIECES // 2:] + right_order[:PIECES // 2]
    for k in range(PIECES):
        start('xr', right_order[k])
        start('xl', left_order[k])
        start('xs', ME, k)
    for rel in INVERSE:
        start('b', rel)

    vt_s[:, head_dim:, :] = jnp.ones((n_heads, vt_s.shape[1] - head_dim, seq), jnp.bfloat16)

    def project(rel):
        place = slice(PLACE[rel] * rows, (PLACE[rel] + 1) * rows)
        xr = h_ref[...] if rel == ME else x_v[rel]
        qk = jnp.dot(xr, wqk_ref[...], preferred_element_type=jnp.float32)
        q_s[place, :] = qk[:, :pair].astype(jnp.bfloat16)
        k_s[place, :] = qk[:, pair:].astype(jnp.bfloat16)
        vt = lax.dot_general(wvt_ref[...], xr, NT, preferred_element_type=jnp.float32).astype(jnp.bfloat16)
        for h in range(n_heads):
            vt_s[h, :head_dim, place] = vt[h * head_dim:(h + 1) * head_dim]

    project(ME)
    for p in range(PIECES):
        recv('xs', ME, p)
    project(SIB)
    for k in range(PIECES):
        recv('xr', right_order[k])
        if k < PIECES // 2:
            start('xrr', right_order[k])
        start('xs', LEFT, right_order[k])
        recv('xl', left_order[k])
        if k < PIECES // 2:
            start('xll', left_order[k])
        start('xs', RIGHT, left_order[k])
        if k == PIECES // 2 - 1:
            for copy in own_copies():
                copy.wait()
            for i in range(2):
                start('wr', TO_RIGHT[i])
                start('wl', TO_LEFT[i])
            for a in ('u', 'd', 'o'):
                start('ws', a)
    project(LEFT)
    project(RIGHT)
    for rel in (LEFT, RIGHT):
        for p in range(PIECES):
            recv('xs', rel, p)
        project(ACROSS[rel])
    for k in range(PIECES // 2):
        recv('xrr', right_order[k])
        start('xs', OPP, right_order[k])
        recv('xll', left_order[k])
        start('xs', OPP, left_order[k])
    project(OPP)
    for p in range(PIECES):
        recv('xs', OPP, p)
    project(SOPP)

    def own(i):
        start('wr', TO_RIGHT[i])
        start('wl', TO_LEFT[i])

    def near(i):
        for kind, relay, rel, c, relayed in (('wr', 'wrr', LEFT, TO_RIGHT[i], RELAY_RIGHT), ('wl', 'wll', RIGHT, TO_LEFT[i], RELAY_LEFT)):
            recv(kind, c)
            if c in relayed:
                start(relay, c)
            if c in Z_CHUNKS:
                start('wz', rel, c)
            start('wfx', rel, c)

    def opposite(chunks):
        for c in chunks:
            recv('wrr' if c in RELAY_RIGHT else 'wll', c)
            if c in Z_CHUNKS:
                start('wz', OPP, c)
            start('wfx', OPP, c)

    def handed(rel, chunks):
        for c in chunks:
            recv('wz', rel, c)
            start('wfz', rel, c)

    ticks = {
        1: [lambda: own(2)],
        2: [lambda: near(0), lambda: own(3)],
        4: [lambda: near(1), lambda: own(4)],
        6: [lambda: near(2), lambda: own(5)],
        7: [lambda: handed(LEFT, ['zu0']), lambda: handed(RIGHT, ['zu1'])],
        8: [lambda: opposite(['zu0', 'zu1']), lambda: own(6)],
        9: [lambda: near(3)],
        10: [lambda: handed(LEFT, ['zd0']), lambda: handed(RIGHT, ['zd1'])],
        11: [lambda: opposite(['zd0', 'zd1'])],
        12: [lambda: near(4)],
        14: [lambda: opposite(['cu', 'co'])],
        15: [lambda: handed(OPP, ['zu0', 'zu1'])],
    }
    for i, rel in enumerate(ORDER[:-1]):
        ticks.setdefault(2 * i + 3, []).insert(0, lambda rel=rel: start('o', rel))

    n_tiles = seq // qt
    n_chunks = seq // kc

    def tile(j, carry):
        for when, actions in ticks.items():
            @pl.when(j == when)
            def _(actions=actions):
                for action in actions:
                    action()
        q = q_s[pl.ds(pl.multiple_of(j * qt, qt), qt), :]
        lane = lax.broadcasted_iota(jnp.int32, q.shape, 1)
        zero = jnp.zeros_like(q)
        qm = jnp.concatenate([jnp.where(lane < head_dim, q, zero), jnp.where(lane >= head_dim, q, zero)], axis=0)
        mx = jnp.full((8, n_heads * qt), -jnp.inf, jnp.float32)
        for c in range(n_chunks):
            keys = slice(c * kc, (c + 1) * kc)
            s = lax.dot_general(k_s[keys, :], qm, NT, preferred_element_type=jnp.float32)
            s_s[keys, :] = s
            mx = jnp.maximum(mx, jnp.max(s.reshape(kc // 8, 8, s.shape[1]), axis=0))
        m = jnp.max(mx, axis=0, keepdims=True) * scale
        for c in range(n_chunks):
            keys = slice(c * kc, (c + 1) * kc)
            p = jnp.exp2(s_s[keys, :] * scale - m).astype(jnp.bfloat16)
            for h in range(n_heads):
                part = jnp.dot(vt_s[h, :, keys], p[:, h * qt:(h + 1) * qt], preferred_element_type=jnp.float32)
                if c == 0:
                    acc_s[h] = part
                else:
                    acc_s[h] += part
        heads = []
        for h in range(n_heads):
            acc = acc_s[h]
            heads.append(acc[:head_dim] / acc[head_dim:head_dim + 1])
        o_loc[pl.ds(pl.multiple_of(j * qt, qt), qt), :] = jnp.concatenate(heads, axis=0).T.astype(jnp.bfloat16)
        return carry

    lax.fori_loop(0, n_tiles, tile, 0)

    near(5)
    near(6)
    opposite(['cd'])
    handed(LEFT, ['zu1'])
    handed(RIGHT, ['zu0'])
    recv('ws', 'o')
    for rel in (LEFT, RIGHT, OPP):
        recv('wfx', rel, 'co')
    for rel in INVERSE:
        recv('o', rel)
        recv('b', rel)
    bu_v[ME] = b_up_ref[...]
    o_rcv[ME] = o_loc[PLACE[ME] * rows:(PLACE[ME] + 1) * rows, :]
    heads = jnp.concatenate([o_rcv[rel] for rel in range(group_size)], axis=1)
    attn_out = jnp.dot(heads, wo_v[...].reshape(width, width), preferred_element_type=jnp.float32)
    r = res_ref[...].astype(jnp.float32) + attn_out + b_out_ref[layer:layer + 1, :]
    r_ref[...] = r
    h2_s[...] = layer_norm(r, norms_ref[base + 2:base + 3, :], norms_ref[base + 3:base + 4, :])

    def arrive_across(rel):
        for c in X_CHUNKS:
            if c != 'co':
                recv('wfx', rel, c)
        for c in Z_CHUNKS:
            recv('wfz', rel, c)

    def before(rel):
        if rel == SIB:
            recv('ws', 'u')
            recv('ws', 'd')
            handed(OPP, ['zd0', 'zd1'])
        elif rel == LEFT:
            handed(LEFT, ['zd1'])
            handed(RIGHT, ['zd0'])
        elif rel == SLEFT:
            arrive_across(LEFT)
        elif rel == SRIGHT:
            arrive_across(RIGHT)
        elif rel == SOPP:
            arrive_across(OPP)

    @pl.loop(0, group_size)
    def _(block):
        for rel in (SIB, LEFT, SLEFT, SRIGHT, SOPP):
            @pl.when(block == rel)
            def _(rel=rel):
                before(rel)
        hidden = jnp.dot(h2_s[...], wu_v[block], preferred_element_type=jnp.float32) + bu_v[block]
        gelu_out = jax.nn.gelu(hidden, approximate=True).astype(jnp.bfloat16)
        r_ref[...] += jnp.dot(gelu_out, wd_v[block], preferred_element_type=jnp.float32)

    r = r_ref[...] + b_down_ref[layer:layer + 1, :]
    if last:
        hn_ref[...] = r.astype(jnp.bfloat16)
    else:
        r_ref[...] = r
        hn_ref[...] = layer_norm(r, norms_ref[base + 4:base + 5, :], norms_ref[base + 5:base + 6, :])
    for key in KEYS:
        message(key).wait_send()


def run_layer(layer, last, group_size, head_dim, h, res, norms, b_out, b_down, b_up, wqk, wvt, w_out, w_up, w_down, qt=256, kc=512):
    rows, width = h.shape
    ff = w_up.shape[-1]
    seq = rows * group_size
    pair = 2 * head_dim
    anywhere = pl.BlockSpec(memory_space=pl.ANY)
    bf16, f32 = jnp.bfloat16, jnp.float32
    return pl.pallas_call(
        functools.partial(layer_kernel, layer, last, group_size, qt, kc),
        out_shape=(jax.ShapeDtypeStruct((rows, width), f32), jax.ShapeDtypeStruct((rows, width), bf16)),
        in_specs=[whole()] * 8 + [anywhere] * 3,
        out_specs=(whole(), whole()),
        scratch_shapes=[
            pltpu.VMEM((group_size, rows, width), bf16),
            pltpu.VMEM((group_size, pair, width), bf16),
            pltpu.VMEM((group_size, width, ff), bf16),
            pltpu.VMEM((group_size, ff, width), bf16),
            pltpu.VMEM((group_size, 1, ff), f32),
            pltpu.VMEM((seq, pair), bf16),
            pltpu.VMEM((seq, pair), bf16),
            pltpu.VMEM((2, head_dim + 16, seq), bf16),
            pltpu.VMEM((seq, 2 * qt), f32),
            pltpu.VMEM((2, head_dim + 16, qt), f32),
            pltpu.VMEM((seq, pair), bf16),
            pltpu.VMEM((group_size, rows, pair), bf16),
            pltpu.VMEM((rows, width), bf16),
            pltpu.SemaphoreType.DMA((len(KEYS),)),
            pltpu.SemaphoreType.DMA((len(KEYS),)),
            pltpu.SemaphoreType.DMA((3,)),
        ],
        compiler_params=pltpu.CompilerParams(collective_id=layer, has_side_effects=True, vmem_limit_bytes=VMEM_LIMIT),
        cost_estimate=pl.CostEstimate(flops=22 * 10**9, bytes_accessed=10 * 2**20, transcendentals=2 * seq * seq),
        name='layer',
    )(h, res, norms, b_out, b_down, b_up, wqk, wvt, w_out, w_up, w_down)


def solution(mesh):
    group_size = mesh.shape['tp']

    def local_layers(hidden_in, norms, w_qkv, w_out, b_out, w_up, b_up, w_down, b_down):
        n_layers, width, slots, heads_loc, head_dim = w_qkv.shape
        pair = heads_loc * head_dim
        norms = norms.reshape(n_layers * 4, width)
        w_out = w_out.reshape(n_layers, pair, width)
        residual = hidden_in[0]
        normed = norm_rows(residual, norms)
        for layer in range(n_layers):
            w_l = w_qkv[layer].reshape(width, slots * pair)
            wqk, wvt = w_l[:, :2 * pair], w_l[:, 2 * pair:].T
            residual, normed = run_layer(layer, layer == n_layers - 1, group_size, head_dim, normed, residual, norms, b_out, b_down,
                                         b_up[layer:layer + 1], wqk, wvt, w_out, w_up, w_down)
        return normed[None]

    in_specs = (P('dp', 'tp', None), P(), P(None, None, None, 'tp', None), P(None, 'tp', None, None), P(), P(None, None, 'tp'), P(None, 'tp'), P(None, 'tp', None), P())
    return jax.shard_map(local_layers, mesh=mesh, in_specs=in_specs, out_specs=P('dp', 'tp', None), check_vma=False)
```

```python
import functools
import jax
import jax.numpy as jnp
from jax import lax
from jax.experimental import pallas as pl
from jax.experimental.pallas import tpu as pltpu
from jax.sharding import PartitionSpec as P

MESH = pl.DeviceIdType.MESH
LN_EPS = 1e-5
LOG2E = 1.4426950408889634
NT = (((1,), (1,)), ((), ()))
VMEM_LIMIT = 63 * 2**20

ME, SIB, LEFT, RIGHT, SLEFT, SRIGHT, OPP, SOPP = range(8)
INVERSE = {SIB: SIB, LEFT: RIGHT, RIGHT: LEFT, OPP: OPP, SLEFT: SRIGHT, SRIGHT: SLEFT, SOPP: SOPP}
ACROSS = {ME: SIB, LEFT: SLEFT, RIGHT: SRIGHT, OPP: SOPP}
ORDER = [OPP, SOPP, LEFT, SLEFT, RIGHT, SRIGHT, SIB, ME]
PLACE = {rel: i for i, rel in enumerate(ORDER)}
PIECES = 4

Z_CHUNKS = ['zu0', 'zu1', 'zd0', 'zd1']
X_CHUNKS = Z_CHUNKS + ['cu', 'cd', 'co']
TO_RIGHT = ['zu0', 'zd0', 'co', 'zu1', 'zd1', 'cu', 'cd']
TO_LEFT = ['zu1', 'zd1', 'co', 'zu0', 'zd0', 'cu', 'cd']
RELAY_RIGHT = ['zu0', 'zd0', 'co']
RELAY_LEFT = ['zu1', 'zd1', 'cu', 'cd']


def layer_norm(rows, gain, shift):
    row_mean = jnp.mean(rows, axis=-1, keepdims=True)
    centred = rows - row_mean
    row_var = jnp.mean(centred * centred, axis=-1, keepdims=True)
    return (centred * lax.rsqrt(row_var + LN_EPS) * gain + shift).astype(jnp.bfloat16)


def whole():
    return pl.BlockSpec(memory_space=pltpu.VMEM)


def norm_kernel(rows_ref, norms_ref, out_ref):
    out_ref[...] = layer_norm(rows_ref[...].astype(jnp.float32), norms_ref[0, 0:1, :], norms_ref[0, 1:2, :])


def norm_rows(rows, norms):
    return pl.pallas_call(
        norm_kernel,
        out_shape=jax.ShapeDtypeStruct(rows.shape, jnp.bfloat16),
        in_specs=[whole()] * 2,
        out_specs=whole(),
        cost_estimate=pl.CostEstimate(flops=10 * rows.size, bytes_accessed=4 * rows.size, transcendentals=0),
        name='norm_rows',
    )(rows, norms)


def message_keys():
    keys = []
    for p in range(PIECES):
        keys += [('xr', p), ('xl', p), ('xs', ME, p)]
        keys += [('xs', rel, p) for rel in (LEFT, RIGHT, OPP)]
        keys += [('xrr', p)] if p < PIECES // 2 else [('xll', p)]
    keys += [('wr', c) for c in X_CHUNKS] + [('wl', c) for c in X_CHUNKS]
    keys += [('wrr', c) for c in RELAY_RIGHT] + [('wll', c) for c in RELAY_LEFT]
    keys += [('ws', a) for a in ('u', 'd', 'o')]
    for rel in (LEFT, RIGHT, OPP):
        keys += [('wfx', rel, c) for c in X_CHUNKS]
        keys += [('wz', rel, c) for c in Z_CHUNKS] + [('wfz', rel, c) for c in Z_CHUNKS]
    keys += [('o', rel) for rel in INVERSE] + [('b', rel) for rel in INVERSE]
    return keys


KEYS = {key: i for i, key in enumerate(message_keys())}


def layer_kernel(layer, last, group_size, qt, kc, h_ref, res_ref, norms_ref, b_out_ref, b_down_ref, b_up_ref, wqkv_ref,
                 w_out_ref, w_up_ref, w_down_ref, r_ref, hn_ref,
                 x_v, wo_v, wu_v, wd_v, bu_v, q_s, k_s, vt_s, s_s, acc_s, o_loc, o_rcv, h2_s, wvt_s, send_sems, recv_sems, own_sems):
    rows, width = h_ref.shape
    ff = w_up_ref.shape[-1]
    seq = q_s.shape[0]
    pair = q_s.shape[1]
    n_heads = 2
    head_dim = pair // n_heads
    scale = head_dim ** -0.5 * LOG2E

    me = lax.axis_index('tp')
    chip, core = me // 2, me % 2
    n_chips = group_size // 2
    parity = lax.axis_index('dp') % 2
    partner = lax.axis_index('dp') + 1 - 2 * parity

    def at(step, flip):
        return {'tp': 2 * ((chip + step) % n_chips) + (1 - core if flip else core)}

    far = n_chips // 2
    device = {SIB: at(0, True), LEFT: at(n_chips - 1, False), RIGHT: at(1, False), OPP: at(far, False),
              SLEFT: at(n_chips - 1, True), SRIGHT: at(1, True), SOPP: at(far, True)}
    pair_device = {'dp': partner, 'tp': me}

    piece_rows = rows // PIECES
    up_z, down_z = width * 7 // 32, ff * 7 // 32

    def x_at(rel, p):
        ref = h_ref if rel == ME else x_v.at[rel]
        return ref.at[p * piece_rows:(p + 1) * piece_rows, :]

    def w_at(rel, c, par):
        if c == 'co':
            return wo_v.at[rel]
        if c == 'cu':
            return wu_v.at[rel, 4 * up_z:, :]
        if c == 'cd':
            return wd_v.at[rel, 4 * down_z:, :]
        i = int(c[2])
        if c[1] == 'u':
            return wu_v.at[rel, pl.ds(pl.multiple_of(par * (2 * up_z) + i * up_z, 16), up_z), :]
        return wd_v.at[rel, pl.ds(pl.multiple_of(par * (2 * down_z) + i * down_z, 16), down_z), :]

    def message(key, receiving=False):
        kind = key[0]
        here, there = parity, 1 - parity
        if kind == 'xr':
            src, dst, dev = x_at(ME, key[1]), x_at(LEFT, key[1]), device[RIGHT]
        elif kind == 'xl':
            src, dst, dev = x_at(ME, key[1]), x_at(RIGHT, key[1]), device[LEFT]
        elif kind == 'xrr':
            src, dst, dev = x_at(LEFT, key[1]), x_at(OPP, key[1]), device[RIGHT]
        elif kind == 'xll':
            src, dst, dev = x_at(RIGHT, key[1]), x_at(OPP, key[1]), device[LEFT]
        elif kind == 'xs':
            src, dst, dev = x_at(key[1], key[2]), x_at(ACROSS[key[1]], key[2]), device[SIB]
        elif kind == 'wr':
            src, dst, dev = w_at(ME, key[1], here), w_at(LEFT, key[1], here), device[RIGHT]
        elif kind == 'wl':
            src, dst, dev = w_at(ME, key[1], here), w_at(RIGHT, key[1], here), device[LEFT]
        elif kind == 'wrr':
            src, dst, dev = w_at(LEFT, key[1], here), w_at(OPP, key[1], here), device[RIGHT]
        elif kind == 'wll':
            src, dst, dev = w_at(RIGHT, key[1], here), w_at(OPP, key[1], here), device[LEFT]
        elif kind == 'ws':
            ref = {'u': wu_v, 'd': wd_v, 'o': wo_v}[key[1]]
            src, dst, dev = ref.at[ME], ref.at[SIB], device[SIB]
        elif kind == 'wfx':
            src, dst, dev = w_at(key[1], key[2], here), w_at(ACROSS[key[1]], key[2], here), device[SIB]
        elif kind == 'wz':
            par = there if receiving else here
            src, dst, dev = w_at(key[1], key[2], par), w_at(key[1], key[2], par), pair_device
        elif kind == 'wfz':
            src, dst, dev = w_at(key[1], key[2], there), w_at(ACROSS[key[1]], key[2], there), device[SIB]
        elif kind == 'o':
            src = o_loc.at[PLACE[key[1]] * rows:(PLACE[key[1]] + 1) * rows, :]
            dst, dev = o_rcv.at[INVERSE[key[1]]], device[key[1]]
        else:
            src, dst, dev = b_up_ref, bu_v.at[INVERSE[key[1]]], device[key[1]]
        i = KEYS[key]
        return pltpu.make_async_remote_copy(src_ref=src, dst_ref=dst, send_sem=send_sems.at[i], recv_sem=recv_sems.at[i],
                                            device_id=dev, device_id_type=MESH)

    def start(*key):
        message(key).start()

    def recv(*key):
        message(key, True).wait_recv()

    def own_copies():
        return [pltpu.make_async_copy(w_up_ref.at[layer], wu_v.at[ME], own_sems.at[0]),
                pltpu.make_async_copy(w_down_ref.at[layer], wd_v.at[ME], own_sems.at[1]),
                pltpu.make_async_copy(w_out_ref.at[layer], wo_v.at[ME], own_sems.at[2])]

    for copy in own_copies():
        copy.start()
    barrier = pltpu.get_barrier_semaphore()
    peers = list(device.values()) + [pair_device]
    for dev in peers:
        pl.semaphore_signal(barrier, inc=1, device_id=dev, device_id_type=MESH)
    pl.semaphore_wait(barrier, len(peers))

    right_order = list(range(PIECES))
    left_order = right_order[PIECES // 2:] + right_order[:PIECES // 2]
    for k in range(PIECES):
        start('xr', right_order[k])
        start('xl', left_order[k])
        start('xs', ME, k)
    for rel in INVERSE:
        start('b', rel)

    wvt_s[...] = wqkv_ref[:, 2 * pair:].T
    vt_s[:, head_dim:, :] = jnp.ones((n_heads, vt_s.shape[1] - head_dim, seq), jnp.bfloat16)

    def own(i):
        start('wr', TO_RIGHT[i])
        start('wl', TO_LEFT[i])

    def near(i):
        for kind, relay, rel, c, relayed in (('wr', 'wrr', LEFT, TO_RIGHT[i], RELAY_RIGHT), ('wl', 'wll', RIGHT, TO_LEFT[i], RELAY_LEFT)):
            recv(kind, c)
            if c in relayed:
                start(relay, c)
            if c in Z_CHUNKS:
                start('wz', rel, c)
            start('wfx', rel, c)

    def opposite(chunks):
        for c in chunks:
            recv('wrr' if c in RELAY_RIGHT else 'wll', c)
            if c in Z_CHUNKS:
                start('wz', OPP, c)
            start('wfx', OPP, c)

    def handed(rel, chunks):
        for c in chunks:
            recv('wz', rel, c)
            start('wfz', rel, c)

    def project(rel):
        place = slice(PLACE[rel] * rows, (PLACE[rel] + 1) * rows)
        xr = h_ref[...] if rel == ME else x_v[rel]
        qk = jnp.dot(xr, wqkv_ref[:, :2 * pair], preferred_element_type=jnp.float32)
        q_s[place, :] = qk[:, :pair].astype(jnp.bfloat16)
        k_s[place, :] = qk[:, pair:].astype(jnp.bfloat16)
        vt = lax.dot_general(wvt_s[...], xr, NT, preferred_element_type=jnp.float32).astype(jnp.bfloat16)
        for h in range(n_heads):
            vt_s[h, :head_dim, place] = vt[h * head_dim:(h + 1) * head_dim]

    project(ME)
    for p in range(PIECES):
        recv('xs', ME, p)
    project(SIB)
    for k in range(PIECES):
        recv('xr', right_order[k])
        if k < PIECES // 2:
            start('xrr', right_order[k])
        start('xs', LEFT, right_order[k])
        recv('xl', left_order[k])
        if k < PIECES // 2:
            start('xll', left_order[k])
        start('xs', RIGHT, left_order[k])
        if k == PIECES // 2 - 1:
            for copy in own_copies():
                copy.wait()
            for i in range(2):
                own(i)
            for a in ('u', 'd', 'o'):
                start('ws', a)
    project(LEFT)
    project(RIGHT)
    for rel in (LEFT, RIGHT):
        for p in range(PIECES):
            recv('xs', rel, p)
        project(ACROSS[rel])
    for k in range(PIECES // 2):
        recv('xrr', right_order[k])
        start('xs', OPP, right_order[k])
        recv('xll', left_order[k])
        start('xs', OPP, left_order[k])
    project(OPP)
    for p in range(PIECES):
        recv('xs', OPP, p)
    project(SOPP)

    ticks = {
        0: [lambda: near(0), lambda: own(2)],
        2: [lambda: near(1), lambda: own(3)],
        4: [lambda: near(2), lambda: own(4)],
        5: [lambda: handed(LEFT, ['zu0']), lambda: handed(RIGHT, ['zu1'])],
        6: [lambda: opposite(['zu0', 'zu1'])],
        7: [lambda: own(5)],
        8: [lambda: near(3), lambda: handed(LEFT, ['zd0']), lambda: handed(RIGHT, ['zd1'])],
        10: [lambda: opposite(['zd0', 'zd1']), lambda: own(6)],
        12: [lambda: near(4), lambda: opposite(['co'])],
        14: [lambda: handed(OPP, ['zu0', 'zu1'])],
    }
    for i, rel in enumerate(ORDER[:-1]):
        ticks.setdefault(2 * i + 3, []).insert(0, lambda rel=rel: start('o', rel))

    n_tiles = seq // qt
    n_chunks = seq // kc

    def tile(j, carry):
        for when, actions in ticks.items():
            @pl.when(j == when)
            def _(actions=actions):
                for action in actions:
                    action()
        q = q_s[pl.ds(pl.multiple_of(j * qt, qt), qt), :]
        lane = lax.broadcasted_iota(jnp.int32, q.shape, 1)
        zero = jnp.zeros_like(q)
        qm = jnp.concatenate([jnp.where(lane < head_dim, q, zero), jnp.where(lane >= head_dim, q, zero)], axis=0)
        mx = jnp.full((8, n_heads * qt), -jnp.inf, jnp.float32)
        for c in range(n_chunks):
            keys = slice(c * kc, (c + 1) * kc)
            s = lax.dot_general(k_s[keys, :], qm, NT, preferred_element_type=jnp.float32)
            s_s[keys, :] = s
            mx = jnp.maximum(mx, jnp.max(s.reshape(kc // 8, 8, s.shape[1]), axis=0))
        m = jnp.max(mx, axis=0, keepdims=True) * scale
        for c in range(n_chunks):
            keys = slice(c * kc, (c + 1) * kc)
            p = jnp.exp2(s_s[keys, :] * scale - m).astype(jnp.bfloat16)
            for h in range(n_heads):
                part = jnp.dot(vt_s[h, :, keys], p[:, h * qt:(h + 1) * qt], preferred_element_type=jnp.float32)
                if c == 0:
                    acc_s[h] = part
                else:
                    acc_s[h] += part
        heads = []
        for h in range(n_heads):
            acc = acc_s[h]
            heads.append(acc[:head_dim] / acc[head_dim:head_dim + 1])
        o_loc[pl.ds(pl.multiple_of(j * qt, qt), qt), :] = jnp.concatenate(heads, axis=0).T.astype(jnp.bfloat16)
        return carry

    lax.fori_loop(0, n_tiles, tile, 0)

    recv('ws', 'o')
    for rel in (LEFT, RIGHT, OPP):
        recv('wfx', rel, 'co')
    for rel in INVERSE:
        recv('o', rel)
        recv('b', rel)
    bu_v[ME] = b_up_ref[...]
    o_rcv[ME] = o_loc[PLACE[ME] * rows:(PLACE[ME] + 1) * rows, :]
    heads = jnp.concatenate([o_rcv[rel] for rel in range(group_size)], axis=1)
    attn_out = jnp.dot(heads, wo_v[...].reshape(width, width), preferred_element_type=jnp.float32)
    r = res_ref[...].astype(jnp.float32) + attn_out + b_out_ref[layer:layer + 1, :]
    r_ref[...] = r
    h2_s[...] = layer_norm(r, norms_ref[layer, 2:3, :], norms_ref[layer, 3:4, :])

    near(5)
    near(6)

    def arrive_across(rel):
        for c in X_CHUNKS:
            if c != 'co':
                recv('wfx', rel, c)
        for c in Z_CHUNKS:
            recv('wfz', rel, c)

    def before(rel):
        if rel == SIB:
            handed(LEFT, ['zu1'])
            handed(RIGHT, ['zu0'])
            recv('ws', 'u')
            recv('ws', 'd')
            opposite(['cu'])
        elif rel == LEFT:
            opposite(['cd'])
            handed(LEFT, ['zd1'])
            handed(RIGHT, ['zd0'])
        elif rel == SLEFT:
            handed(OPP, ['zd0', 'zd1'])
            arrive_across(LEFT)
        elif rel == SRIGHT:
            arrive_across(RIGHT)
        elif rel == SOPP:
            arrive_across(OPP)

    @pl.loop(0, group_size)
    def _(block):
        for rel in (SIB, LEFT, SLEFT, SRIGHT, SOPP):
            @pl.when(block == rel)
            def _(rel=rel):
                before(rel)
        hidden = jnp.dot(h2_s[...], wu_v[block], preferred_element_type=jnp.float32) + bu_v[block]
        gelu_out = jax.nn.gelu(hidden, approximate=True).astype(jnp.bfloat16)
        r_ref[...] += jnp.dot(gelu_out, wd_v[block], preferred_element_type=jnp.float32)

    r = r_ref[...] + b_down_ref[layer:layer + 1, :]
    if last:
        hn_ref[...] = r.astype(jnp.bfloat16)
    else:
        r_ref[...] = r
        hn_ref[...] = layer_norm(r, norms_ref[layer + 1, 0:1, :], norms_ref[layer + 1, 1:2, :])
    for key in KEYS:
        message(key).wait_send()


def run_layer(layer, last, group_size, head_dim, h, res, norms, b_out, b_down, b_up, wqkv, w_out, w_up, w_down, qt=256, kc=512):
    rows, width = h.shape
    ff = w_up.shape[-1]
    seq = rows * group_size
    pair = 2 * head_dim
    anywhere = pl.BlockSpec(memory_space=pl.ANY)
    bf16, f32 = jnp.bfloat16, jnp.float32
    return pl.pallas_call(
        functools.partial(layer_kernel, layer, last, group_size, qt, kc),
        out_shape=(jax.ShapeDtypeStruct((rows, width), f32), jax.ShapeDtypeStruct((rows, width), bf16)),
        in_specs=[whole()] * 7 + [anywhere] * 3,
        out_specs=(whole(), whole()),
        scratch_shapes=[
            pltpu.VMEM((group_size, rows, width), bf16),
            pltpu.VMEM((group_size, pair, width), bf16),
            pltpu.VMEM((group_size, width, ff), bf16),
            pltpu.VMEM((group_size, ff, width), bf16),
            pltpu.VMEM((group_size, 1, ff), f32),
            pltpu.VMEM((seq, pair), bf16),
            pltpu.VMEM((seq, pair), bf16),
            pltpu.VMEM((2, head_dim + 16, seq), bf16),
            pltpu.VMEM((seq, 2 * qt), f32),
            pltpu.VMEM((2, head_dim + 16, qt), f32),
            pltpu.VMEM((seq, pair), bf16),
            pltpu.VMEM((group_size, rows, pair), bf16),
            pltpu.VMEM((rows, width), bf16),
            pltpu.VMEM((pair, width), bf16),
            pltpu.SemaphoreType.DMA((len(KEYS),)),
            pltpu.SemaphoreType.DMA((len(KEYS),)),
            pltpu.SemaphoreType.DMA((3,)),
        ],
        compiler_params=pltpu.CompilerParams(collective_id=layer, has_side_effects=True, vmem_limit_bytes=VMEM_LIMIT),
        cost_estimate=pl.CostEstimate(flops=22 * 10**9, bytes_accessed=10 * 2**20, transcendentals=2 * seq * seq),
        name='layer',
    )(h, res, norms, b_out, b_down, b_up, wqkv, w_out, w_up, w_down)


def solution(mesh):
    group_size = mesh.shape['tp']

    def local_layers(hidden_in, norms, w_qkv, w_out, b_out, w_up, b_up, w_down, b_down):
        n_layers, width, slots, heads_loc, head_dim = w_qkv.shape
        pair = heads_loc * head_dim
        w_out = w_out.reshape(n_layers, pair, width)
        residual = hidden_in[0]
        normed = norm_rows(residual, norms)
        for layer in range(n_layers):
            wqkv = w_qkv[layer].reshape(width, slots * pair)
            residual, normed = run_layer(layer, layer == n_layers - 1, group_size, head_dim, normed, residual, norms, b_out, b_down,
                                         b_up[layer:layer + 1], wqkv, w_out, w_up, w_down)
        return normed[None]

    in_specs = (P('dp', 'tp', None), P(), P(None, None, None, 'tp', None), P(None, 'tp', None, None), P(), P(None, None, 'tp'), P(None, 'tp'), P(None, 'tp', None), P())
    return jax.shard_map(local_layers, mesh=mesh, in_specs=in_specs, out_specs=P('dp', 'tp', None), check_vma=False)
```
